768 devices in a mesh: lon: 32 (over x, z_hi, core), lat: 24 (over z_lo, y).
Axes of the slice: x: 4, y: 8, z: 12 (z_hi: 4, z_lo: 3; z = z_hi * 3 + z_lo), core: 2. Of those that a mesh axis runs over, the one named last changes fastest.
Arguments:
- fields: bfloat16 [144, 384, 2, 192], P('lat', 'lon'), may hold values from -6 to 6
- cotangent: bfloat16 [144, 384, 2, 192], P('lat', 'lon'), may hold values from -6 to 6
- qkv_plain: bfloat16 [192, 576], replicated, may hold values from -0.4375 to 0.4375
- proj_plain: bfloat16 [192, 192], replicated, may hold values from -0.4375 to 0.4375
- up_plain: bfloat16 [192, 768], replicated, may hold values from -0.4375 to 0.4375
- down_plain: bfloat16 [768, 192], replicated, may hold values from -0.21875 to 0.21875
- bias_plain: bfloat16 [24, 1, 6, 144, 144], P('lat'), may hold values from -4 to 4
- qkv_shift: bfloat16 [192, 576], replicated, may hold values from -0.4375 to 0.4375
- proj_shift: bfloat16 [192, 192], replicated, may hold values from -0.4375 to 0.4375
- up_shift: bfloat16 [192, 768], replicated, may hold values from -0.4375 to 0.4375
- down_shift: bfloat16 [768, 192], replicated, may hold values from -0.21875 to 0.21875
- bias_shift: bfloat16 [24, 1, 6, 144, 144], P('lat'), may hold values from -4 to 4
Outputs:
- result: bfloat16 [144, 384, 2, 192], P('lat', 'lon')
- grad_fields: bfloat16 [144, 384, 2, 192], P('lat', 'lon')
- grad_qkv_plain: float32 [192, 576], P(None, 'lat')
- grad_proj_plain: float32 [192, 192], P(None, 'lat')
- grad_up_plain: float32 [192, 768], P(None, 'lat')
- grad_down_plain: float32 [768, 192], P(None, 'lat')
- grad_qkv_shift: float32 [192, 576], P(None, 'lat')
- grad_proj_shift: float32 [192, 192], P(None, 'lat')
- grad_up_shift: float32 [192, 768], P(None, 'lat')
- grad_down_shift: float32 [768, 192], P(None, 'lat')
The draws below stay inside these ranges and needn't reach their ends.
All inputs are finite; a program needn't handle non-finite values.
Results may differ from the reference program's by a relative error of at most 0.04.
Values may be sent and summed in bfloat16 or wider, within the bound.
No kernel may reach another device: no remote copies, remote signals or barrier semaphores. Data moves between devices by JAX's collectives and lax.ppermute only.
A program may use at most 64 MiB of HBM per device.

```python
import jax
import jax.numpy as jnp
from jax import lax

D = 192
HEADS = 6
FF = 768
WLAT = 6
WLON = 12
WPL = 2
PL = 2
WIN = 144
NLAT = 144
NLON = 384
NWLAT = 24


def strengthened(values, key, source, target, shards_of, factor):
    def block_of(position):
        return (jnp.arange(values.shape[position]) // (values.shape[position] // shards_of)).reshape((-1,) + (1,) * (values.ndim - 1 - position))

    near = jax.random.permutation(key, shards_of)[block_of(target)]
    far = (block_of(target) + shards_of // 2) % shards_of
    return jnp.where((block_of(source) == near) | (block_of(source) == far), factor * values, values)


def steps_of(key, extent, split, low, top_value):
    level = 1.0
    for axis_at, parts in split:
        draws = jax.random.uniform(jax.random.fold_in(jax.random.fold_in(key, 6), axis_at), (parts,), jnp.float32, low / len(split), top_value / len(split))
        level = level * jnp.repeat(jnp.exp(draws), extent[axis_at] // parts).reshape((-1,) + (1,) * (len(extent) - 1 - axis_at))
    return level


def scatter_about(rng, dims, scale, most, cuts=(), held_as=jnp.bfloat16):
    gain = steps_of(rng, dims, cuts, -0.22, 0.18) if cuts else 1.0
    array = jax.random.normal(rng, dims, jnp.float32) * scale * gain
    return jnp.minimum(jnp.maximum(array, -most), most).astype(held_as)


def gaussian_with(rng, shape, scale, limit, pieces, heavy, kind=jnp.bfloat16):
    entries = scale * jax.random.normal(rng, shape, jnp.float32)
    if pieces:
        entries = entries * steps_of(rng, shape, pieces, -0.22, 0.18)
    return jnp.clip(strengthened(entries, jax.random.fold_in(rng, 3), *heavy), -limit, limit).astype(kind)


def setup_inputs(seed: int = 0) -> dict:
    streams_of = jax.random.split(jax.random.key(seed), 13)
    return {
        "fields": scatter_about(streams_of[0], (NLAT, NLON, PL, D), 1.0, 6.0, ((0, 24), (1, 32))),
        "cotangent": gaussian_with(streams_of[1], (NLAT, NLON, PL, D), 1.0, 6.0, ((0, 24), (1, 32)), (0, 3, 24, 2.25)),
        "qkv_plain": scatter_about(streams_of[2], (D, 3 * D), D ** -0.5, 0.4375),
        "proj_plain": scatter_about(streams_of[3], (D, D), D ** -0.5, 0.4375),
        "up_plain": scatter_about(streams_of[4], (D, FF), D ** -0.5, 0.4375),
        "down_plain": scatter_about(streams_of[5], (FF, D), FF ** -0.5, 0.21875),
        "bias_plain": scatter_about(streams_of[6], (NWLAT, PL // WPL, HEADS, WIN, WIN), 1.0, 4.0, ((0, 24),)),
        "qkv_shift": scatter_about(streams_of[7], (D, 3 * D), D ** -0.5, 0.4375),
        "proj_shift": scatter_about(streams_of[8], (D, D), D ** -0.5, 0.4375),
        "up_shift": scatter_about(streams_of[9], (D, FF), D ** -0.5, 0.4375),
        "down_shift": scatter_about(streams_of[10], (FF, D), FF ** -0.5, 0.21875),
        "bias_shift": scatter_about(streams_of[11], (NWLAT, PL // WPL, HEADS, WIN, WIN), 1.0, 4.0, ((0, 24),)),
    }


EPS = 1e-05

def normalize(values):
    average = lax.optimization_barrier(jnp.mean(values, axis=-1, keepdims=True))
    centred = values - average
    variance = lax.optimization_barrier(jnp.mean(centred * centred, axis=-1, keepdims=True))
    return centred * lax.rsqrt(variance + EPS)

def to_windows(grid):
    lat_cells, lon_cells, levels = grid.shape[:3]
    trailing = grid.shape[3:]
    blocked = grid.reshape((lat_cells // WLAT, WLAT, lon_cells // WLON, WLON, levels // WPL, WPL) + trailing)
    ordering = (0, 2, 4, 1, 3, 5) + tuple(range(6, 6 + len(trailing)))
    permuted = jnp.transpose(blocked, ordering)
    return permuted.reshape((lat_cells // WLAT, lon_cells // WLON * (levels // WPL), WLAT * WLON * WPL) + trailing)

def from_windows(wins, lat_cells, lon_cells, levels):
    trailing = wins.shape[3:]
    blocked = wins.reshape((lat_cells // WLAT, lon_cells // WLON, levels // WPL, WLAT, WLON, WPL) + trailing)
    ordering = (0, 3, 1, 4, 2, 5) + tuple(range(6, 6 + len(trailing)))
    permuted = jnp.transpose(blocked, ordering)
    return permuted.reshape((lat_cells, lon_cells, levels) + trailing)

def block_forward(inputs, weights, bias, groups):
    w_qkv, w_proj, w_up, w_down = weights
    bands, per_band, window_size, width = inputs.shape
    pressure_wins = bias.shape[1]
    heads = bias.shape[2]
    head_size = width // heads
    flat_in = inputs.reshape(-1, width).astype(jnp.float32)
    normed = normalize(flat_in).astype(jnp.bfloat16)
    mixed = jnp.dot(normed, w_qkv, preferred_element_type=jnp.float32).astype(jnp.bfloat16)
    mixed = mixed.reshape(bands, per_band, window_size, 3, heads, head_size)
    query_part = mixed[:, :, :, 0]
    key_part = mixed[:, :, :, 1]
    value_part = mixed[:, :, :, 2]
    scores = jnp.einsum('bnqhd,bnkhd->bnhqk', query_part.astype(jnp.float32), key_part.astype(jnp.float32))
    scores = scores.reshape(bands, per_band // pressure_wins, pressure_wins, heads, window_size, window_size)
    scores = scores * head_size ** (-0.5) + bias[:, None].astype(jnp.float32)
    scores = scores.reshape(bands, per_band, heads, window_size, window_size)
    allowed = (groups[:, :, :, None] == groups[:, :, None, :])[:, :, None].astype(jnp.float32)
    weighted = jnp.exp(scores) * allowed
    probs = weighted / lax.optimization_barrier(jnp.sum(weighted, axis=-1, keepdims=True))
    probs_low = probs.astype(jnp.bfloat16)
    attended = jnp.einsum('bnhqk,bnkhd->bnqhd', probs_low.astype(jnp.float32), value_part.astype(jnp.float32))
    attended = attended.astype(jnp.bfloat16).reshape(-1, width)
    after_attn = (flat_in + jnp.dot(attended, w_proj, preferred_element_type=jnp.float32)).astype(jnp.bfloat16)
    after_f32 = after_attn.astype(jnp.float32)
    normed_two = normalize(after_f32).astype(jnp.bfloat16)
    pre_act = jnp.dot(normed_two, w_up, preferred_element_type=jnp.float32)
    activated = jax.nn.gelu(pre_act).astype(jnp.bfloat16)
    outputs = (after_f32 + jnp.dot(activated, w_down, preferred_element_type=jnp.float32)).astype(jnp.bfloat16)
    saved = (flat_in, normed, query_part, key_part, value_part, probs, probs_low, attended, after_f32, normed_two, pre_act, activated)
    return (outputs.reshape(inputs.shape), saved)

def block_backward(saved, cotangent, weights):
    w_qkv, w_proj, w_up, w_down = weights
    flat_in, normed, query_part, key_part, value_part, probs, probs_low, attended, after_f32, normed_two, pre_act, activated = saved
    width = flat_in.shape[1]
    scale = query_part.shape[-1] ** (-0.5)
    grad_out = cotangent.reshape(-1, width)
    grad_down = jnp.dot(activated.T, grad_out, preferred_element_type=jnp.float32)
    grad_act = jnp.dot(grad_out, w_down.T, preferred_element_type=jnp.float32)
    unused_one, gelu_back = jax.vjp(jax.nn.gelu, pre_act)
    grad_pre = gelu_back(grad_act)[0].astype(jnp.bfloat16)
    grad_up = jnp.dot(normed_two.T, grad_pre, preferred_element_type=jnp.float32)
    grad_norm_two = jnp.dot(grad_pre, w_up.T, preferred_element_type=jnp.float32)
    unused_two, second_back = jax.vjp(normalize, after_f32)
    grad_after = grad_out.astype(jnp.float32) + second_back(grad_norm_two)[0]
    grad_after_low = grad_after.astype(jnp.bfloat16)
    grad_proj = jnp.dot(attended.T, grad_after_low, preferred_element_type=jnp.float32)
    grad_attended = jnp.dot(grad_after_low, w_proj.T, preferred_element_type=jnp.float32).astype(jnp.bfloat16)
    grad_attended = grad_attended.reshape(query_part.shape).astype(jnp.float32)
    grad_value = jnp.einsum('bnhqk,bnqhd->bnkhd', probs_low.astype(jnp.float32), grad_attended).astype(jnp.bfloat16)
    grad_probs = jnp.einsum('bnqhd,bnkhd->bnhqk', grad_attended, value_part.astype(jnp.float32))
    grad_scores = (probs * (grad_probs - lax.optimization_barrier(jnp.sum(grad_probs * probs, axis=-1, keepdims=True))) * scale).astype(jnp.bfloat16)
    grad_query = jnp.einsum('bnhqk,bnkhd->bnqhd', grad_scores.astype(jnp.float32), key_part.astype(jnp.float32)).astype(jnp.bfloat16)
    grad_key = jnp.einsum('bnhqk,bnqhd->bnkhd', grad_scores.astype(jnp.float32), query_part.astype(jnp.float32)).astype(jnp.bfloat16)
    grad_mixed = jnp.stack([grad_query, grad_key, grad_value], axis=3).reshape(-1, 3 * width)
    grad_qkv = jnp.dot(normed.T, grad_mixed, preferred_element_type=jnp.float32)
    grad_normed = jnp.dot(grad_mixed, w_qkv.T, preferred_element_type=jnp.float32)
    unused_three, first_back = jax.vjp(normalize, flat_in)
    grad_in = (grad_after + first_back(grad_normed)[0]).astype(jnp.bfloat16)
    return (grad_in.reshape(cotangent.shape), (grad_qkv, grad_proj, grad_up, grad_down))

def roll_grid(grid, direction):
    return jnp.roll(grid, (direction * (WLAT // 2), direction * (WLON // 2), direction * (WPL // 2)), axis=(0, 1, 2))

def run_forward(grid, weights, bias, groups):
    wins = to_windows(grid)
    group_wins = to_windows(groups)

    def one_band(items):
        outputs, unused = block_forward(items[0][None], weights, items[1][None], items[2][None])
        return outputs[0]
    outs = lax.map(one_band, (wins, bias, group_wins))
    return from_windows(outs, NLAT, NLON, PL)

def run_backward(grid, cot_grid, weights, bias, groups):
    wins = to_windows(grid)
    cot_wins = to_windows(cot_grid)
    group_wins = to_windows(groups)
    zeros = tuple((jnp.zeros(weight.shape, jnp.float32) for weight in weights))

    def one_band(carry, items):
        unused, saved = block_forward(items[0][None], weights, items[1][None], items[3][None])
        grad_in, grads = block_backward(saved, items[2][None], weights)
        return (jax.tree.map(jnp.add, carry, grads), grad_in[0])
    totals, grad_wins = lax.scan(one_band, zeros, (wins, bias, cot_wins, group_wins))
    return (from_windows(grad_wins, NLAT, NLON, PL), totals)

def reference(fields, cotangent, qkv_plain, proj_plain, up_plain, down_plain, bias_plain, qkv_shift, proj_shift, up_shift, down_shift, bias_shift):
    plain = (qkv_plain, proj_plain, up_plain, down_plain)
    shifted = (qkv_shift, proj_shift, up_shift, down_shift)
    lat_index = jnp.arange(NLAT, dtype=jnp.int32)[:, None, None]
    level_index = jnp.arange(PL, dtype=jnp.int32)[None, None, :]
    group_shift = (lat_index >= NLAT - WLAT // 2).astype(jnp.int32) * 2 + (level_index >= PL - WPL // 2).astype(jnp.int32)
    group_shift = jnp.broadcast_to(group_shift, (NLAT, NLON, PL))
    group_plain = jnp.zeros((NLAT, NLON, PL), jnp.int32)
    first_out = run_forward(fields, plain, bias_plain, group_plain)
    moved_in = roll_grid(first_out, -1)
    second_out = run_forward(moved_in, shifted, bias_shift, group_shift)
    result = roll_grid(second_out, 1)
    moved_cot = roll_grid(cotangent, -1)
    grad_moved, grads_shift = run_backward(moved_in, moved_cot, shifted, bias_shift, group_shift)
    grad_first = roll_grid(grad_moved, 1)
    grad_fields, grads_plain = run_backward(fields, grad_first, plain, bias_plain, group_plain)
    factor = (NLAT * NLON * PL) ** (-0.5)
    return (result, grad_fields, grads_plain[0] * factor, grads_plain[1] * factor, grads_plain[2] * factor, grads_plain[3] * factor, grads_shift[0] * factor, grads_shift[1] * factor, grads_shift[2] * factor, grads_shift[3] * factor)
```

```python
import functools

import jax
import jax.numpy as jnp
import numpy as np
from jax import lax
from jax.experimental import pallas as pl
from jax.experimental.pallas import tpu as pltpu
from jax.sharding import PartitionSpec as P

WLAT = 6
WLON = 12
WPL = 2
WIN = WLAT * WLON * WPL
HEADS = 6
D = 192
HEAD = D // HEADS
FF = 768
PIECE = 40
EPS = 1e-05
F32 = jnp.float32
BF16 = jnp.bfloat16
VMEM = pl.BlockSpec(memory_space=pltpu.VMEM)
SMEM = pl.BlockSpec(memory_space=pltpu.SMEM)


def placements():
    half_lat, half_lon = WLAT // 2, WLON // 2

    def at(i, j, l):
        return (i * WLON + j) * WPL + l

    own = np.zeros((WIN, WIN), np.float32)
    take = np.zeros((3, PIECE, WIN), np.float32)
    put = np.zeros((3, WIN, PIECE), np.float32)
    corners = (
        (half_lat, 0, 0, half_lon),
        (0, half_lon, half_lat, 0),
        (half_lat, half_lon, 0, 0),
    )
    for i in range(half_lat):
        for j in range(half_lon):
            for l in range(WPL):
                own[at(i, j, 1 - l), at(i + half_lat, j + half_lon, l)] = 1
                row = (i * half_lon + j) * WPL + l
                for k, (di, dj, si, sj) in enumerate(corners):
                    take[k, row, at(i + si, j + sj, l)] = 1
                    put[k, at(i + di, j + dj, 1 - l), row] = 1
    return own, take, put


OWN, TAKE, PUT = placements()


def dot(a, b, dims=((1,), (0,))):
    return lax.dot_general(a, b, (dims, ((), ())), preferred_element_type=F32)


def dot_nt(a, b):
    return dot(a, b, ((1,), (1,)))


def dot_tn(a, b):
    return dot(a, b, ((0,), (0,)))


def normalize(values):
    average = jnp.mean(values, axis=-1, keepdims=True)
    centred = values - average
    variance = jnp.mean(centred * centred, axis=-1, keepdims=True)
    inverse = lax.rsqrt(variance + EPS)
    return centred * inverse, inverse


def normalize_back(normed, inverse, grad):
    mean_grad = jnp.mean(grad, axis=-1, keepdims=True)
    mean_both = jnp.mean(grad * normed, axis=-1, keepdims=True)
    return inverse * (grad - mean_grad - normed * mean_both)


GELU_A = np.float32(np.sqrt(2 / np.pi))
GELU_B = np.float32(0.044715)


def head_masks():
    lanes = lax.broadcasted_iota(jnp.int32, (WIN, D), 1)
    return [(lanes >= h * HEAD) & (lanes < (h + 1) * HEAD) for h in range(HEADS)]


def spread(values, masks):
    zero = jnp.zeros_like(values)
    return jnp.concatenate([jnp.where(m, values, zero) for m in masks], axis=0)


def gather_heads(stacked, masks):
    total = None
    for h, m in enumerate(masks):
        part = jnp.where(m, stacked[h * WIN : (h + 1) * WIN], 0.0)
        total = part if total is None else total + part
    return total


def forward(x, w_qkv, w_proj, w_up, w_down, bias, allowed):
    masks = head_masks()
    x32 = x.astype(F32)
    normed, inverse = normalize(x32)
    h = normed.astype(BF16)
    mixed = dot(h, w_qkv[...]).astype(BF16)
    q, k, v = mixed[:, :D], mixed[:, D : 2 * D], mixed[:, 2 * D :]
    q_heads = spread(q.astype(F32), [m for m in masks]).astype(BF16)
    scores = dot_nt(q_heads, k) * np.float32(HEAD ** (-0.5))
    scores = scores.reshape(HEADS, WIN, WIN) + bias[...].astype(F32)
    weighted = jnp.exp(scores)
    if allowed is not None:
        weighted = weighted * allowed[None]
    probs = weighted / jnp.sum(weighted, axis=-1, keepdims=True)
    probs = probs.reshape(HEADS * WIN, WIN)
    probs_low = probs.astype(BF16)
    o = gather_heads(dot(probs_low, v), masks).astype(BF16)
    x1 = (x32 + dot(o, w_proj[...])).astype(BF16).astype(F32)
    normed2, inverse2 = normalize(x1)
    h2 = normed2.astype(BF16)
    pre = dot(h2, w_up[...])
    cubed = pre * pre * pre
    tanh = jnp.tanh(GELU_A * (pre + GELU_B * cubed))
    u = (0.5 * pre * (1.0 + tanh)).astype(BF16)
    out = (x1 + dot(u, w_down[...])).astype(BF16)
    saved = (
        masks, normed, inverse, h, q_heads, k, v, probs, probs_low,
        o, normed2, inverse2, h2, pre, tanh, u,
    )
    return out, saved


def backward(saved, c, w_qkv, w_proj, w_up, w_down, emit):
    (
        masks, normed, inverse, h, q_heads, k, v, probs, probs_low,
        o, normed2, inverse2, h2, pre, tanh, u,
    ) = saved
    c32 = c.astype(F32)
    emit_down = dot_tn(c, u)
    du = dot_nt(c, w_down[...])
    slope = 0.5 * (1.0 + tanh) + (0.5 * GELU_A) * pre * (1.0 - tanh * tanh) * (
        1.0 + (3.0 * GELU_B) * pre * pre
    )
    dg = (du * slope).astype(BF16)
    emit_up = dot_tn(dg, h2)
    dh2 = dot_nt(dg, w_up[...])
    dx1 = c32 + normalize_back(normed2, inverse2, dh2)
    dx1_low = dx1.astype(BF16)
    emit_proj = dot_tn(dx1_low, o)
    do = dot_nt(dx1_low, w_proj[...]).astype(BF16)
    do_heads = spread(do.astype(F32), masks).astype(BF16)
    dv = dot_tn(probs_low, do_heads)
    dp = dot_nt(do_heads, v)
    inner = jnp.sum(dp * probs, axis=-1, keepdims=True)
    ds = (probs * (dp - inner) * np.float32(HEAD ** (-0.5))).astype(BF16)
    dq = gather_heads(dot(ds, k), masks)
    dk = dot_tn(ds, q_heads)
    dm = jnp.concatenate([dq, dk, dv], axis=1).astype(BF16)
    emit_qkv = dot_tn(dm, h)
    dh = dot_nt(dm, w_qkv[...])
    dx = (dx1 + normalize_back(normed, inverse, dh)).astype(BF16)
    emit(emit_qkv, emit_proj, emit_up, emit_down)
    return dx


def store_grads(ref, shares, qkv, proj, up, down):
    a, b, c, d = (g.shape[0] // shares for g in (qkv, proj, up, down))
    for s in range(shares):
        first = jnp.concatenate(
            [qkv[s * a : (s + 1) * a], proj[s * b : (s + 1) * b]], axis=0
        )
        second = up[s * c : (s + 1) * c]
        both = jnp.concatenate(
            [
                first[:, :128],
                second[:, :128],
                jnp.concatenate([first[:, 128:], second[:, 128:]], axis=1),
            ],
            axis=0,
        )
        ref[s, 0:96, :] = both.astype(BF16)
        last = down[s * d : (s + 1) * d]
        ref[s, 96:144, :] = jnp.concatenate(
            [last[:, 128 * t : 128 * (t + 1)] for t in range(6)], axis=0
        ).astype(BF16)


def plain_kernel(x, cot, w_qkv, w_proj, w_up, w_down, bias, take, y_out, piece_out):
    y, _ = forward(x[...], w_qkv, w_proj, w_up, w_down, bias, None)
    y_out[...] = y
    for k in range(3):
        piece_out[k, 0:PIECE, :] = dot(take[k], y).astype(BF16)
        piece_out[k, PIECE : 2 * PIECE, :] = dot(take[k], cot[...]).astype(BF16)


def shift_kernel(
    shares, last_row, y, cot, from_lat, from_lon, from_diag,
    w_qkv, w_proj, w_up, w_down, bias, own, own_t, put, put_t,
    nat_out, piece_out, grads_out,
):
    x = dot(own[...], y[...])
    c = dot(own[...], cot[...])
    for k, got in enumerate((from_lat, from_lon, from_diag)):
        x = x + dot(put[k], got[0:PIECE, :])
        c = c + dot(put[k], got[PIECE : 2 * PIECE, :])
    rows = lax.broadcasted_iota(jnp.int32, (WIN, WIN), 0)
    cols = lax.broadcasted_iota(jnp.int32, (WIN, WIN), 1)
    middle = WIN // 2
    apart = ((rows >= middle) ^ (cols >= middle)).astype(jnp.int32) * last_row[0]
    apart = apart + ((rows ^ cols) & 1)
    allowed = (apart == 0).astype(F32)
    result, saved = forward(x.astype(BF16), w_qkv, w_proj, w_up, w_down, bias, allowed)
    emit = functools.partial(store_grads, grads_out, shares)
    grad = backward(saved, c.astype(BF16), w_qkv, w_proj, w_up, w_down, emit)
    nat_out[0] = dot(own_t[...], result).astype(BF16)
    nat_out[1] = dot(own_t[...], grad).astype(BF16)
    for k in range(3):
        piece_out[k, 0:PIECE, :] = dot(put_t[k], result).astype(BF16)
        piece_out[k, PIECE : 2 * PIECE, :] = dot(put_t[k], grad).astype(BF16)


def final_kernel(
    shares, core, x, nat, from_lat, from_lon, from_diag,
    w_qkv, w_proj, w_up, w_down, bias, take_t, shift_grads,
    result_out, grad_out, send_out, keep_out, grads,
):
    result = nat[0].astype(F32)
    c = nat[1].astype(F32)
    for k, got in enumerate((from_lat, from_lon, from_diag)):
        result = result + dot(take_t[k], got[0:PIECE, :])
        c = c + dot(take_t[k], got[PIECE : 2 * PIECE, :])
    result_out[...] = result.astype(BF16)
    _, saved = forward(x[...], w_qkv, w_proj, w_up, w_down, bias, None)
    emit = functools.partial(store_grads, grads, shares)
    grad_out[...] = backward(
        saved, c.astype(BF16), w_qkv, w_proj, w_up, w_down, emit
    )

    @pl.when(core[0] == 0)
    def _():
        keep_out[...] = grads[...]
        send_out[...] = shift_grads[...]

    @pl.when(core[0] != 0)
    def _():
        keep_out[...] = shift_grads[...]
        send_out[...] = grads[...]


def add_kernel(a, b, out):
    out[...] = (a[...].astype(F32) + b[...].astype(F32)).astype(BF16)


def call(body, shapes, specs, name, flops, scratch=()):
    return pl.pallas_call(
        body,
        out_shape=tuple(jax.ShapeDtypeStruct(s, d) for s, d in shapes),
        in_specs=specs,
        out_specs=tuple(VMEM for _ in shapes),
        scratch_shapes=scratch,
        name=name,
        cost_estimate=pl.CostEstimate(flops=flops, bytes_accessed=4000000, transcendentals=300000),
        compiler_params=pltpu.CompilerParams(vmem_limit_bytes=48 * 1024 * 1024),
    )


def exchanged(pieces, steps):
    n_lat, n_lon = lax.axis_size("lat"), lax.axis_size("lon")
    lat = [(i, (i + steps) % n_lat) for i in range(n_lat)]
    lon = [(i, (i + steps) % n_lon) for i in range(n_lon)]
    both = [
        (j * n_lat + i, (j + steps) % n_lon * n_lat + (i + steps) % n_lat)
        for i in range(n_lat)
        for j in range(n_lon)
    ]
    return (
        lax.ppermute(pieces[2], ("lon", "lat"), both),
        lax.ppermute(pieces[1], "lon", lon),
        lax.ppermute(pieces[0], "lat", lat),
    )[::-1]


def reduced(keep, send):
    n_lon = lax.axis_size("lon")
    pair = [(i, i ^ 1) for i in range(n_lon)]
    got = lax.ppermute(send, "lon", pair)
    mine = (keep.astype(F32) + got.astype(F32)).astype(BF16)
    parts = lax.all_to_all(mine, "lat", 0, 0, tiled=True)
    share = jnp.sum(parts.astype(F32), axis=0).astype(BF16)
    for step in (8, 16, 2, 4):
        other = lax.ppermute(share, "lon", [(i, i ^ step) for i in range(n_lon)])
        share = (share.astype(F32) + other.astype(F32)).astype(BF16)
    return share, lax.ppermute(share, "lon", pair)


def unpacked(share, factor, a, b, c, d):
    share = share.astype(F32) * factor
    first = jnp.concatenate([share[0 : a + b], share[a + b + c : a + b + c + c, :64]], axis=1)
    second = jnp.concatenate([share[a + b : a + b + c], share[a + b + c : a + b + c + c, 64:]], axis=1)
    last = share[96:144].reshape(6, d, 128).transpose(1, 0, 2).reshape(d, FF)
    return first[:a].T, first[a:].T, second.T, last.T


def local(
    fields,
    cotangent,
    qkv_plain,
    proj_plain,
    up_plain,
    down_plain,
    bias_plain,
    qkv_shift,
    proj_shift,
    up_shift,
    down_shift,
    bias_shift,
):
    n_lat, n_lon = lax.axis_size("lat"), lax.axis_size("lon")
    plain = (qkv_plain, proj_plain, up_plain, down_plain, bias_plain.reshape(HEADS, WIN, WIN))
    shifted = (qkv_shift, proj_shift, up_shift, down_shift, bias_shift.reshape(HEADS, WIN, WIN))
    x = fields.reshape(WIN, D)
    cot = cotangent.reshape(WIN, D)
    own, take, put = (jnp.asarray(m, BF16) for m in (OWN, TAKE, PUT))
    own_t = jnp.asarray(OWN.T, BF16)
    take_t, put_t = (jnp.asarray(m.transpose(0, 2, 1), BF16) for m in (TAKE, PUT))
    last_row = (lax.axis_index("lat") == n_lat - 1).astype(jnp.int32).reshape(1)
    core = (lax.axis_index("lon") % 2).astype(jnp.int32).reshape(1)
    packed = (n_lat, WIN, 128)
    tokens = (WIN, D)
    moved = (3, 2 * PIECE, D)

    y, pieces = call(
        plain_kernel, ((tokens, BF16), (moved, BF16)), [VMEM] * 8, "plain", 150000000
    )(x, cot, *plain, take)
    got = exchanged(pieces, -1)
    nat, pieces, shift_grads = call(
        functools.partial(shift_kernel, n_lat),
        (((2,) + tokens, BF16), (moved, BF16), (packed, BF16)),
        [SMEM] + [VMEM] * 14,
        "shift",
        450000000,
    )(last_row, y, cot, *got, *shifted, own, own_t, put, put_t)
    got = exchanged(pieces, 1)
    result, grad_fields, send, keep = call(
        functools.partial(final_kernel, n_lat),
        ((tokens, BF16), (tokens, BF16), (packed, BF16), (packed, BF16)),
        [SMEM] + [VMEM] * 12,
        "final",
        450000000,
        (pltpu.VMEM(packed, BF16),),
    )(core, x, nat, *got, *plain, take_t, shift_grads)
    mine, other = reduced(keep, send)
    is_first = (core == 0)[:, None]
    plain_share = jnp.where(is_first, mine, other)
    shift_share = jnp.where(is_first, other, mine)
    factor = float(WIN * n_lat * n_lon) ** (-0.5)
    sizes = tuple(n // n_lat for n in (3 * D, D, FF, D))
    return (
        result.reshape(fields.shape),
        grad_fields.reshape(fields.shape),
        *unpacked(plain_share, factor, *sizes),
        *unpacked(shift_share, factor, *sizes),
    )


def solution(mesh):
    placed = (
        P("lat", "lon", None, None),
        P("lat", "lon", None, None),
        P(),
        P(),
        P(),
        P(),
        P("lat", None, None, None, None),
        P(),
        P(),
        P(),
        P(),
        P("lat", None, None, None, None),
    )
    return jax.shard_map(
        local,
        mesh=mesh,
        in_specs=placed,
        out_specs=(
            P("lat", "lon", None, None),
            P("lat", "lon", None, None),
            P(None, "lat"),
            P(None, "lat"),
            P(None, "lat"),
            P(None, "lat"),
            P(None, "lat"),
            P(None, "lat"),
            P(None, "lat"),
            P(None, "lat"),
        ),
        check_vma=False,
    )
```
